512 devices in a mesh: sector: 32 (over z_lo, x, core), term: 16 (over z_hi, y).
Axes of the slice: x: 4, y: 8, z: 8 (z_hi: 2, z_lo: 4; z = z_hi * 4 + z_lo), core: 2. Of those that a mesh axis runs over, the one named last changes fastest.
Arguments:
- wave: float32 [32, 512, 512], P('sector', 'term'), may hold values from -12 to 12
- left_ops: bfloat16 [64, 32, 512, 512], P('term', 'sector'), may hold values from -4 to 4
- right_ops: bfloat16 [64, 32, 512, 512], P('term', 'sector'), may hold values from -4 to 4
- charges: int32 [64], replicated, may hold values from -1 to 1, as said below
- diag: float32 [32, 512, 512], P('sector', 'term'), may hold values from 0.5 to 8
Outputs:
- psi_out: float32 [32, 512, 512], P('sector', 'term')
The draws below stay inside these ranges and needn't reach their ends.
Inputs may be any that keep to these rules, and one draw needn't show every extreme that they name: `charges`: exactly (65) // 2 terms have charge 0; at least one term has charge 1 and at least one has charge -1.
All inputs are finite; a program needn't handle non-finite values.
Results may differ from the reference program's by a relative error of at most 0.0085.
Values may be sent and summed in bfloat16 or wider, within the bound.
A program may use at most 64 MiB of HBM per device.

```python
import jax
import jax.numpy as jnp
from jax import lax

SECT = 512
STEPS = 3
SECTORS = 32
TERMS = 64


def sector_gains(key):
    gain_key = jax.random.fold_in(key, 7)
    uniform_draw = jax.random.uniform(gain_key, (SECTORS,), jnp.float32)
    lowest, highest = (0.75, 6.0)
    strength = jnp.exp(jnp.log(lowest) + uniform_draw * (jnp.log(highest) - jnp.log(lowest)))
    return jnp.sqrt(2.0 * strength / TERMS)


def environment(key, salt):
    sector_gain = sector_gains(key)
    noise_key = jax.random.fold_in(key, salt)
    noise_part = jnp.clip(jax.random.normal(noise_key, (TERMS, SECTORS, SECT, SECT), jnp.float32), -6.0, 6.0)
    noise_part = noise_part / jnp.sqrt(jnp.float32(SECT))
    identity = jnp.eye(SECT, dtype=jnp.float32)
    blocks = noise_part + sector_gain[None, :, None, None] * identity[None, None]
    return blocks.astype(jnp.bfloat16)


def draw_left_ops(key, part):
    return environment(key, 11)


def draw_right_ops(key, part):
    return environment(key, 13)


def draw_wave(key, part):
    scale_key = jax.random.fold_in(key, 23)
    entry_key = jax.random.fold_in(key, 29)
    uniform_draw = jax.random.uniform(scale_key, (SECTORS,), jnp.float32)
    amplitude = jnp.exp(jnp.log(0.5) + uniform_draw * (jnp.log(2.0) - jnp.log(0.5)))
    entries = jnp.clip(jax.random.normal(entry_key, (SECTORS, SECT, SECT), jnp.float32), -6.0, 6.0)
    return (entries * amplitude[:, None, None]).astype(jnp.float32)


def draw_charges(key, part):
    ordering = jax.random.permutation(jax.random.fold_in(key, 17), TERMS)
    sign_draw = 2 * jax.random.randint(jax.random.fold_in(key, 19), (TERMS,), 0, 2) - 1
    zero_count = (TERMS + 1) // 2
    position = jnp.arange(TERMS, dtype=jnp.int32)
    by_position = jnp.where(position < zero_count, 0, jnp.where(position == zero_count, 1, jnp.where(position == zero_count + 1, -1, sign_draw)))
    charge_list = jnp.zeros((TERMS,), jnp.int32).at[ordering].set(by_position.astype(jnp.int32))
    return charge_list.astype(jnp.int32)


def block_scale(key, shape, pieces, least, top_value):
    factor_of, own = 1.0, jax.random.fold_in(key, 6)
    for dim, shards_of in pieces:
        heights = jnp.exp(jax.random.uniform(jax.random.fold_in(own, dim), (shards_of,), jnp.float32, least / len(pieces), top_value / len(pieces)))
        factor_of = factor_of * jnp.repeat(heights, shape[dim] // shards_of).reshape([-1 if axis == dim else 1 for axis in range(len(shape))])
    return factor_of


def setup_inputs(seed: int = 0) -> dict:
    key_of = jax.random.split(jax.random.key(seed), 6)
    return {
        "wave": draw_wave(jax.random.fold_in(key_of[5], 71), 0),
        "left_ops": draw_left_ops(jax.random.fold_in(key_of[5], 71), 0),
        "right_ops": draw_right_ops(jax.random.fold_in(key_of[5], 71), 0),
        "charges": draw_charges(jax.random.fold_in(key_of[5], 71), 0),
        "diag": jnp.clip(0.5 + 7.5 * jax.random.uniform(key_of[4], (SECTORS, SECT, SECT), jnp.float32) ** block_scale(key_of[4], (SECTORS, SECT, SECT), ((0, 32), (1, 16)), -0.2, 0.2), 0.5, 8.0),
    }


def reference(wave, left_ops, right_ops, charges, diag):
    psi = wave
    zero_block = jnp.zeros((1, SECT, SECT), jnp.bfloat16)
    for step in range(STEPS):
        wb = psi.astype(jnp.bfloat16)
        lower = jnp.concatenate([zero_block, wb[:-1]], axis=0)
        upper = jnp.concatenate([wb[1:], zero_block], axis=0)

        def add_term(acc, items):
            left, right, charge = items
            source = jnp.where(charge == 1, lower, jnp.where(charge == -1, upper, wb))
            inner = jnp.einsum('sij,sjk->sik', left.astype(jnp.float32), source.astype(jnp.float32)).astype(jnp.bfloat16)
            image = jnp.einsum('sij,skj->sik', inner.astype(jnp.float32), right.astype(jnp.float32))
            return (acc + image, None)
        hpsi, unused = lax.scan(add_term, jnp.zeros(psi.shape, jnp.float32), (left_ops, right_ops, charges))
        theta = jnp.sum(psi * hpsi) / jnp.sum(psi * psi)
        fresh = psi - (hpsi - theta * psi) / jnp.maximum(jnp.abs(diag - theta), 1.0)
        psi = fresh / jnp.sqrt(jnp.mean(fresh * fresh) + 1e-06)
    return psi
```

```python
import functools

import jax
import jax.numpy as jnp
from jax import lax
from jax.experimental import pallas as pl
from jax.experimental.pallas import tpu as pltpu
from jax.sharding import PartitionSpec as P

STEPS = 3
ROWS = 32
BF16, F32 = jnp.bfloat16, jnp.float32
LONG = ((0, 0), (1, 1))
SHORT = ((0, 1), (1, 0))


def wrapped(value, count):
    return lax.rem(value + count, count)


def lane_sums(x):
    x = jnp.sum(x, axis=0, keepdims=True)
    return x[:, :128] + x[:, 128:256] + x[:, 256:384] + x[:, 384:]


def kernel(
    total_size,
    charges,
    wave,
    diag,
    left_hbm,
    right_hbm,
    out,
    left,
    right,
    blocks,
    image,
    rs_out,
    rs_in,
    z_out,
    z_in,
    f,
    dg,
    sc_out,
    sc_in,
    load_sem,
    first_send,
    first_recv,
    ag_send,
    ag_recv,
    nb_send,
    nb_recv,
    rs_send,
    rs_recv,
    z_send,
    z_recv,
    sc_send,
    sc_recv,
):
    s, t = lax.axis_index("sector"), lax.axis_index("term")
    sectors = lax.axis_size("sector")
    y, zh = lax.rem(t, 8), lax.div(t, 8)
    xc, zl = lax.rem(s, 8), lax.div(s, 8)
    z = zh * 4 + zl

    def remote(src, dst, send, recv, sector, term):
        return pltpu.make_async_remote_copy(
            src_ref=src,
            dst_ref=dst,
            send_sem=send,
            recv_sem=recv,
            device_id={"sector": sector, "term": term},
            device_id_type=pl.DeviceIdType.MESH,
        )

    def arrived(ref, sem):
        pltpu.make_async_copy(ref, ref, sem).wait()

    def peer(phase, offset):
        if phase == 0:
            return s, zh * 8 + lax.rem(y + offset, 8)
        if phase == 1:
            return zl * 8 + lax.rem(xc + offset, 8), t
        other = lax.rem(z + offset, 8)
        return lax.rem(other, 4) * 8 + xc, lax.div(other, 4) * 8 + y

    place = (y, xc, z)
    has_lower, has_upper = s > 0, s < sectors - 1

    loads = [
        pltpu.make_async_copy(left_hbm, left, load_sem.at[0]),
        pltpu.make_async_copy(right_hbm, right, load_sem.at[1]),
    ]
    for load in loads:
        load.start()

    barrier = pltpu.get_barrier_semaphore()

    def greet(sector, term):
        pl.semaphore_signal(
            barrier,
            inc=1,
            device_id={"sector": sector, "term": term},
            device_id_type=pl.DeviceIdType.MESH,
        )

    for phase in range(3):
        for offset in range(1, 8):
            greet(*peer(phase, offset))
    far_lower = jnp.logical_and(xc == 0, has_lower)
    far_upper = jnp.logical_and(xc == 7, has_upper)

    @pl.when(far_lower)
    def _():
        greet(s - 1, t)

    @pl.when(far_upper)
    def _():
        greet(s + 1, t)

    f[zh] = wave[0]
    dg[zh] = diag[0]
    blocks[0, 1, zh, y] = wave[0].astype(BF16)

    @pl.when(s == 0)
    def _():
        for k in range(STEPS):
            blocks[k, 2] = jnp.zeros(blocks.shape[2:], BF16)

    @pl.when(s == sectors - 1)
    def _():
        for k in range(STEPS):
            blocks[k, 0] = jnp.zeros(blocks.shape[2:], BF16)

    first_square = lane_sums(jnp.square(wave[0]))
    pl.semaphore_wait(barrier, 21 + far_lower.astype(jnp.int32) + far_upper.astype(jnp.int32))

    zt = (1 - zh) * 8 + y
    ring_to = (zh * 8 + wrapped(y + 1, 8), zh * 8 + wrapped(y - 1, 8))
    first = [
        remote(blocks.at[0, 1, zh, y], blocks.at[0, 1, zh, y], first_send.at[0], first_recv.at[0], s, zt),
        remote(wave.at[0], f.at[zh], first_send.at[1], first_recv.at[1], s, zt),
        remote(diag.at[0], dg.at[zh], first_send.at[2], first_recv.at[2], s, zt),
    ]
    for copy in first:
        copy.start()
    first[0].wait_recv()

    def position(d, distance):
        return wrapped(y - distance if d == 0 else y + distance, 8)

    def destination(d, distance):
        return wrapped(y + distance if d == 0 else y - distance, 8)

    def hand_on(k, ref_of):
        @pl.when(has_upper)
        def _():
            remote(ref_of(blocks.at[k, 1]), ref_of(blocks.at[k, 2]), nb_send.at[0], nb_recv.at[k, 0], s + 1, t).start()

        @pl.when(has_lower)
        def _():
            remote(ref_of(blocks.at[k, 1]), ref_of(blocks.at[k, 0]), nb_send.at[1], nb_recv.at[k, 1], s - 1, t).start()

    def gather(k):
        def ring_copy(d, h, r):
            piece = blocks.at[k, 1, h, position(d, r)]
            return remote(piece, piece, ag_send.at[0], ag_recv.at[k, d, h, r], s, ring_to[d])

        def wait_piece(d, h, r):
            ring_copy(d, h, r).wait_recv()

        for r in range(4):
            for d, h in LONG:
                if r:
                    wait_piece(d, h, r - 1)
                ring_copy(d, h, r).start()
            for d, h in SHORT:
                if r:
                    wait_piece(d, h, r - 1)
                if r < 3:
                    ring_copy(d, h, r).start()
            hand_on(k, lambda ref: ref.at[:, position(0, r)])
            if r:
                hand_on(k, lambda ref: ref.at[:, position(1, r)])
        for d, h in LONG:
            wait_piece(d, h, 3)
        hand_on(k, lambda ref: ref.at[:, position(0, 4)])

        @pl.when(has_lower)
        def _():
            arrived(blocks.at[k, 2], nb_recv.at[k, 0])

        @pl.when(has_upper)
        def _():
            arrived(blocks.at[k, 0], nb_recv.at[k, 1])

    def apply_rows(k, ends):
        total = None
        for i in range(4):
            source = blocks[k, charges[t * 4 + i] + 1].reshape(512, 512)
            rows = jnp.concatenate([left[i, h, e] for e in ends for h in range(2)], axis=0)
            inner = jnp.dot(rows, source, preferred_element_type=F32).astype(BF16)
            term = lax.dot_general(inner, right[i], (((1,), (1,)), ((), ())), preferred_element_type=F32)
            total = term if total is None else total + term
        mine = jnp.concatenate([blocks[k, 1, h, e] for e in ends for h in range(2)], axis=0)
        for j, e in enumerate(ends):
            for h in range(2):
                at = (2 * j + h) * ROWS
                image[h, e] = total[at : at + ROWS]
        return lane_sums(total * mine.astype(F32))

    def pass_on(k, d, h, q):
        where = destination(d, q)
        value = image[h, where]
        if q < (4 if (d, h) in LONG else 3):
            rs_copy(k, d, h, q + 1).wait_recv()
            value = value + rs_in[k, d, h, q].astype(F32)
        rs_out[k, d, h, q - 1] = value.astype(BF16)
        rs_copy(k, d, h, q).start()

    def rs_copy(k, d, h, q):
        return remote(
            rs_out.at[k, d, h, q - 1],
            rs_in.at[k, d, h, q - 1],
            rs_send.at[0],
            rs_recv.at[k, d, h, q - 1],
            s,
            ring_to[d],
        )

    def sum_start(k, phase, values):
        sc_out[k, phase] = values
        sc_in[k, phase, place[phase]] = values
        for offset in range(1, 8):
            remote(
                sc_out.at[k, phase],
                sc_in.at[k, phase, place[phase]],
                sc_send.at[0],
                sc_recv.at[k, phase],
                *peer(phase, offset),
            ).start()

    def sum_end(k, phase):
        arrived(sc_in.at[k, phase, pl.ds(0, 7)], sc_recv.at[k, phase])
        return jnp.sum(sc_in[k, phase], axis=0)

    def pair(cross, square):
        return jnp.concatenate([cross, square], axis=0)

    def step(k, square):
        gather(k)

        @pl.when(k == 0)
        def _():
            for load in loads:
                load.wait()

        cross = apply_rows(k, (destination(0, 4), destination(0, 3)))
        for d, h in LONG:
            pass_on(k, d, h, 4)
        pass_on(k, 0, 1, 3)
        cross += apply_rows(k, (destination(1, 3), destination(0, 2)))
        pass_on(k, 1, 0, 3)
        cross += apply_rows(k, (destination(1, 2), destination(0, 1)))
        for d, h in LONG:
            pass_on(k, d, h, 3)
        cross += apply_rows(k, (destination(1, 1), y))
        sum_start(k, 0, pair(cross, square))
        for d, h in SHORT + LONG:
            pass_on(k, d, h, 2)
        sum_start(k, 1, sum_end(k, 0))
        for d, h in SHORT + LONG:
            pass_on(k, d, h, 1)
        for h in range(2):
            for d in range(2):
                rs_copy(k, d, h, 1).wait_recv()
            z_out[k, h] = (image[h, y] + rs_in[k, 0, h, 0].astype(F32) + rs_in[k, 1, h, 0].astype(F32)).astype(BF16)
        across = remote(z_out.at[k], z_in.at[k], z_send.at[0], z_recv.at[k], s, zt)
        across.start()
        sum_start(k, 2, sum_end(k, 1))
        sums = sum_end(k, 2)
        both = jnp.sum(sums, axis=1, keepdims=True)
        cross_total, square_total = both[0:1], both[1:2]
        theta = (cross_total / square_total)[None]
        scale = jnp.where(k == 0, 1.0, 1.0 / jnp.sqrt(square_total / total_size + 1e-06))[None]

        @pl.when(k == 0)
        def _():
            first[1].wait_recv()
            first[2].wait_recv()

        across.wait_recv()
        hpsi = (z_out[k].astype(F32) + z_in[k].astype(F32)) * scale
        psi = f[...] * scale
        fresh = psi - (hpsi - theta * psi) / jnp.maximum(jnp.abs(dg[...] - theta), 1.0)
        f[...] = fresh

        @pl.when(k < STEPS - 1)
        def _():
            blocks[jnp.minimum(k + 1, STEPS - 1), 1, :, y] = fresh.astype(BF16)

        return 0.5 * lane_sums(jnp.square(fresh).reshape(2 * ROWS, 512))

    square = lax.fori_loop(0, STEPS, step, first_square)
    last = pair(square, square)
    for phase in range(3):
        sum_start(STEPS, phase, last)
        last = sum_end(STEPS, phase)
    norm = jnp.sum(last, axis=1, keepdims=True)[1:2]
    out[0] = f[zh] / jnp.sqrt(norm / total_size + 1e-06)

    for copy in first:
        copy.wait_send()
    arrived(rs_in.at[:, :, :, pl.ds(0, 3)], ag_send.at[0])
    arrived(rs_in.at[:, 0, :, pl.ds(0, 1)], ag_send.at[0])
    arrived(rs_in.at[:, :, :, pl.ds(0, 3)], rs_send.at[0])
    arrived(rs_in.at[:, 0, :, pl.ds(0, 1)], rs_send.at[0])
    arrived(z_in, z_send.at[0])
    arrived(sc_in.at[:, :, pl.ds(0, 7)], sc_send.at[0])

    @pl.when(has_upper)
    def _():
        arrived(blocks.at[:, 0], nb_send.at[0])

    @pl.when(has_lower)
    def _():
        arrived(blocks.at[:, 0], nb_send.at[1])


def per_device(wave, left_ops, right_ops, charges, diag):
    total_size = float(lax.axis_size("sector") * 512 * 512)
    vmem = pl.BlockSpec(memory_space=pltpu.VMEM)
    hbm = pl.BlockSpec(memory_space=pl.ANY)
    dma = pltpu.SemaphoreType.DMA
    return pl.pallas_call(
        functools.partial(kernel, total_size),
        out_shape=jax.ShapeDtypeStruct(wave.shape, F32),
        in_specs=[pl.BlockSpec(memory_space=pltpu.SMEM), vmem, vmem, hbm, hbm],
        out_specs=vmem,
        scratch_shapes=[
            pltpu.VMEM((4, 2, 8, ROWS, 512), BF16),
            pltpu.VMEM((4, 512, 512), BF16),
            pltpu.VMEM((STEPS, 3, 2, 8, ROWS, 512), BF16),
            pltpu.VMEM((2, 8, ROWS, 512), F32),
            pltpu.VMEM((STEPS, 2, 2, 4, ROWS, 512), BF16),
            pltpu.VMEM((STEPS, 2, 2, 4, ROWS, 512), BF16),
            pltpu.VMEM((STEPS, 2, ROWS, 512), BF16),
            pltpu.VMEM((STEPS, 2, ROWS, 512), BF16),
            pltpu.VMEM((2, ROWS, 512), F32),
            pltpu.VMEM((2, ROWS, 512), F32),
            pltpu.VMEM((STEPS + 1, 3, 2, 128), F32),
            pltpu.VMEM((STEPS + 1, 3, 8, 2, 128), F32),
            dma((2,)),
            dma((3,)),
            dma((3,)),
            dma((1,)),
            dma((STEPS, 2, 2, 4)),
            dma((2,)),
            dma((STEPS, 2)),
            dma((1,)),
            dma((STEPS, 2, 2, 4)),
            dma((1,)),
            dma((STEPS,)),
            dma((1,)),
            dma((STEPS + 1, 3)),
        ],
        compiler_params=pltpu.CompilerParams(
            collective_id=0, has_side_effects=True, vmem_limit_bytes=48 * 1024 * 1024
        ),
        name="sweep",
    )(
        charges,
        wave,
        diag,
        left_ops.reshape(4, 2, 8, ROWS, 512),
        right_ops.reshape(4, 512, 512),
    )


def solution(mesh):
    in_specs = (
        P("sector", "term", None),
        P("term", "sector", None, None),
        P("term", "sector", None, None),
        P(),
        P("sector", "term", None),
    )
    out_specs = P("sector", "term", None)
    return jax.shard_map(
        per_device, mesh=mesh, in_specs=in_specs, out_specs=out_specs, check_vma=False
    )
```

```python
import functools

import jax
import jax.numpy as jnp
from jax import lax
from jax.experimental import pallas as pl
from jax.experimental.pallas import tpu as pltpu
from jax.sharding import PartitionSpec as P

STEPS = 3
SLOTS = (16, 32)
ROWS = 32
BF16, F32 = jnp.bfloat16, jnp.float32
LONG = ((0, 0), (1, 1))
SHORT = ((0, 1), (1, 0))


def wrapped(value, count):
    return lax.rem(value + count, count)


def lane_sums(x):
    x = jnp.sum(x, axis=0, keepdims=True)
    return x[:, :128] + x[:, 128:256] + x[:, 256:384] + x[:, 384:]


def kernel(
    total_size,
    charges,
    wave_hbm,
    diag_hbm,
    left_hbm,
    right_hbm,
    out,
    left,
    right,
    blocks,
    image,
    rs_out,
    rs_in,
    z_out,
    z_in,
    f,
    dg,
    sc_out,
    sc_in_0,
    sc_in_1,
    load_sem,
    first_send,
    first_recv,
    ag_send,
    ag_recv,
    nb_send,
    nb_recv,
    rs_send,
    rs_recv,
    z_send,
    z_recv,
    sc_send,
    sc_recv,
):
    s, t = lax.axis_index("sector"), lax.axis_index("term")
    sectors = lax.axis_size("sector")
    y, zh = lax.rem(t, 8), lax.div(t, 8)
    core, x, zl = lax.rem(s, 2), lax.rem(lax.div(s, 2), 4), lax.div(s, 8)
    z = zh * 4 + zl

    sc_in = (sc_in_0, sc_in_1)

    def remote(src, dst, send, recv, sector, term):
        return pltpu.make_async_remote_copy(
            src_ref=src,
            dst_ref=dst,
            send_sem=send,
            recv_sem=recv,
            device_id={"sector": sector, "term": term},
            device_id_type=pl.DeviceIdType.MESH,
        )

    def arrived(ref, sem):
        pltpu.make_async_copy(ref, ref, sem).wait()

    def peer(phase, offset):
        if phase == 0:
            other = lax.rem(place[0] + offset, 16)
            return s - core + lax.rem(other, 2), zh * 8 + lax.div(other, 2)
        other = lax.rem(place[1] + offset, 32)
        oz = lax.div(other, 4)
        return (lax.rem(oz, 4) * 4 + lax.rem(other, 4)) * 2 + core, lax.div(oz, 4) * 8 + y

    place = (y * 2 + core, z * 4 + x)
    has_lower, has_upper = s > 0, s < sectors - 1

    own = [
        pltpu.make_async_copy(wave_hbm.at[0], f.at[zh], load_sem.at[2]),
        pltpu.make_async_copy(diag_hbm.at[0], dg.at[zh], load_sem.at[3]),
    ]
    loads = [
        pltpu.make_async_copy(left_hbm, left, load_sem.at[0]),
        pltpu.make_async_copy(right_hbm, right, load_sem.at[1]),
    ]
    for load in own + loads:
        load.start()

    barrier = pltpu.get_barrier_semaphore()

    def greet(sector, term):
        pl.semaphore_signal(
            barrier,
            inc=1,
            device_id={"sector": sector, "term": term},
            device_id_type=pl.DeviceIdType.MESH,
        )

    for phase in range(2):

        def greet_peer(offset, carry, phase=phase):
            greet(*peer(phase, offset))
            return carry

        lax.fori_loop(1, SLOTS[phase], greet_peer, 0)
    zt = (1 - zh) * 8 + y
    ring_to = (zh * 8 + wrapped(y + 1, 8), zh * 8 + wrapped(y - 1, 8))
    skip_to = (zh * 8 + wrapped(y + 2, 8), zh * 8 + wrapped(y - 2, 8))
    cross_to = ((1 - zh) * 8 + wrapped(y + 1, 8), (1 - zh) * 8 + wrapped(y - 1, 8))
    for term in cross_to:
        greet(s, term)
    far_lower = jnp.logical_and(core == 0, has_lower)
    far_upper = jnp.logical_and(core == 1, has_upper)

    @pl.when(far_lower)
    def _():
        greet(s - 1, t)

    @pl.when(far_upper)
    def _():
        greet(s + 1, t)

    @pl.when(s == 0)
    def _():
        for k in range(STEPS):
            blocks[k, 2] = jnp.zeros(blocks.shape[2:], BF16)

    @pl.when(s == sectors - 1)
    def _():
        for k in range(STEPS):
            blocks[k, 0] = jnp.zeros(blocks.shape[2:], BF16)

    for load in own:
        load.wait()
    blocks[0, 1, zh, y] = f[zh].astype(BF16)
    first_square = lane_sums(jnp.square(f[zh]))
    pl.semaphore_wait(barrier, 48 + far_lower.astype(jnp.int32) + far_upper.astype(jnp.int32))

    first = [
        remote(blocks.at[0, 1, zh, y], blocks.at[0, 1, zh, y], first_send.at[0], first_recv.at[0], s, zt),
        remote(f.at[zh], f.at[zh], first_send.at[1], first_recv.at[1], s, zt),
        remote(dg.at[zh], dg.at[zh], first_send.at[2], first_recv.at[2], s, zt),
    ]

    def position(d, distance):
        return wrapped(y - distance if d == 0 else y + distance, 8)

    def destination(d, distance):
        return wrapped(y + distance if d == 0 else y - distance, 8)

    def hand_on(k, ref_of):
        @pl.when(has_upper)
        def _():
            remote(ref_of(blocks.at[k, 1]), ref_of(blocks.at[k, 2]), nb_send.at[0], nb_recv.at[k, 0], s + 1, t).start()

        @pl.when(has_lower)
        def _():
            remote(ref_of(blocks.at[k, 1]), ref_of(blocks.at[k, 0]), nb_send.at[1], nb_recv.at[k, 1], s - 1, t).start()

    def gather(k):
        def ring_copy(d, h, r):
            piece = blocks.at[k, 1, h, position(d, r)]
            return remote(piece, piece, ag_send.at[0], ag_recv.at[k, d, h, r], s, ring_to[d])

        def wait_piece(d, h, r):
            ring_copy(d, h, r).wait_recv()

        def start_skip(d, h):
            piece = blocks.at[k, 1, h, position(d, 2)]
            remote(piece, piece, ag_send.at[0], ag_recv.at[k, d, h, 3], s, skip_to[d]).start()

        @pl.when(k == 0)
        def _():
            piece = blocks.at[0, 1, zh, y]
            for d in range(2):
                remote(piece, piece, ag_send.at[0], ag_recv.at[0, d, zh, 0], s, cross_to[d]).start()
            first[0].start()
            for d in range(2):
                remote(piece, piece, ag_send.at[0], ag_recv.at[0, d, zh, 0], s, ring_to[d]).start()
            for copy in first[1:]:
                copy.start()

        @pl.when(k > 0)
        def _():
            for d, h in LONG + SHORT:
                ring_copy(d, h, 0).start()
            hand_on(k, lambda ref: ref.at[:, y])

        for d, h in LONG + SHORT:
            wait_piece(d, h, 0)
            ring_copy(d, h, 1).start()

        @pl.when(k == 0)
        def _():
            first[0].wait_recv()
            hand_on(k, lambda ref: ref.at[:, y])

        for d in range(2):
            hand_on(k, lambda ref: ref.at[:, position(d, 1)])
        for d, h in LONG:
            wait_piece(d, h, 1)
            start_skip(d, h)
            ring_copy(d, h, 2).start()
        for d, h in SHORT:
            wait_piece(d, h, 1)
            ring_copy(d, h, 2).start()
        for d in range(2):
            hand_on(k, lambda ref: ref.at[:, position(d, 2)])
        for d in range(2):
            for h in range(2):
                wait_piece(d, h, 2)
            hand_on(k, lambda ref: ref.at[:, position(d, 3)])
        for d, h in LONG:
            wait_piece(d, h, 3)
        hand_on(k, lambda ref: ref.at[:, position(0, 4)])

        @pl.when(has_lower)
        def _():
            arrived(blocks.at[k, 2], nb_recv.at[k, 0])

        @pl.when(has_upper)
        def _():
            arrived(blocks.at[k, 0], nb_recv.at[k, 1])

    def apply_rows(k, ends):
        total = None
        for i in range(4):
            source = blocks[k, charges[t * 4 + i] + 1].reshape(512, 512)
            rows = jnp.concatenate([left[i, h, e] for e in ends for h in range(2)], axis=0)
            inner = jnp.dot(rows, source, preferred_element_type=F32).astype(BF16)
            term = lax.dot_general(inner, right[i], (((1,), (1,)), ((), ())), preferred_element_type=F32)
            total = term if total is None else total + term
        mine = jnp.concatenate([blocks[k, 1, h, e] for e in ends for h in range(2)], axis=0)
        for j, e in enumerate(ends):
            for h in range(2):
                at = (2 * j + h) * ROWS
                image[h, e] = total[at : at + ROWS]
        return lane_sums(total * mine.astype(F32))

    def pass_on(k, d, h, q):
        value = image[h, destination(d, q)]
        if q == 2:
            rs_copy(k, d, h, 3).wait_recv()
            value = value + rs_in[k, d, h, 2].astype(F32)
            if (d, h) in LONG:
                rs_copy(k, d, h, 4).wait_recv()
                value = value + rs_in[k, d, h, 3].astype(F32)
        rs_out[k, d, h, q - 1] = value.astype(BF16)
        rs_copy(k, d, h, q).start()

    def rs_copy(k, d, h, q):
        return remote(
            rs_out.at[k, d, h, q - 1],
            rs_in.at[k, d, h, q - 1],
            rs_send.at[0],
            rs_recv.at[k, d, h, q - 1],
            s,
            skip_to[d] if q % 2 == 0 else ring_to[d],
        )

    def sum_start(k, phase, values):
        sums = sc_in[phase]
        sc_out[k, phase] = values
        sums[k, place[phase]] = values

        def send(offset, carry):
            remote(
                sc_out.at[k, phase],
                sums.at[k, place[phase]],
                sc_send.at[0],
                sc_recv.at[k, phase],
                *peer(phase, offset),
            ).start()
            return carry

        lax.fori_loop(1, SLOTS[phase], send, 0)

    def sum_end(k, phase):
        sums = sc_in[phase]
        arrived(sums.at[k, pl.ds(0, SLOTS[phase] - 1)], sc_recv.at[k, phase])
        return jnp.sum(sums[k], axis=0)

    def pair(cross, square):
        lane = lax.broadcasted_iota(jnp.int32, (1, 128), 1)
        cross, square = (jnp.sum(v, axis=1, keepdims=True) for v in (cross, square))
        return jnp.where(lane < 64, cross, square)

    def step(k, square):
        gather(k)

        @pl.when(k == 0)
        def _():
            for load in loads:
                load.wait()

        cross = apply_rows(k, (destination(0, 4), destination(0, 3)))
        for d, h in LONG:
            pass_on(k, d, h, 4)
        for h in range(2):
            pass_on(k, 0, h, 3)
        cross += apply_rows(k, (destination(1, 3), destination(0, 2)))
        for h in range(2):
            pass_on(k, 1, h, 3)
        cross += apply_rows(k, (destination(1, 2), destination(0, 1)))
        for h in range(2):
            pass_on(k, 0, h, 1)
        cross += apply_rows(k, (destination(1, 1), y))
        for h in range(2):
            pass_on(k, 1, h, 1)
        sum_start(k, 0, pair(cross, square))
        for d, h in SHORT + LONG:
            pass_on(k, d, h, 2)
        sum_start(k, 1, sum_end(k, 0))
        for h in range(2):
            total = image[h, y]
            for d in range(2):
                for q in (1, 2):
                    rs_copy(k, d, h, q).wait_recv()
                    total = total + rs_in[k, d, h, q - 1].astype(F32)
            z_out[k, h] = total.astype(BF16)
        across = remote(z_out.at[k], z_in.at[k], z_send.at[0], z_recv.at[k], s, zt)
        across.start()
        sums = sum_end(k, 1)
        cross_total, square_total = sums[:, 0:1], sums[:, 64:65]
        theta = (cross_total / square_total)[None]
        scale = jnp.where(k == 0, 1.0, 1.0 / jnp.sqrt(square_total / total_size + 1e-06))[None]

        @pl.when(k == 0)
        def _():
            first[1].wait()
            first[2].wait()

        across.wait_recv()
        hpsi = (z_out[k].astype(F32) + z_in[k].astype(F32)) * scale
        psi = f[...] * scale
        fresh = psi - (hpsi - theta * psi) / jnp.maximum(jnp.abs(dg[...] - theta), 1.0)
        f[...] = fresh

        @pl.when(k < STEPS - 1)
        def _():
            blocks[jnp.minimum(k + 1, STEPS - 1), 1, :, y] = fresh.astype(BF16)

        return 0.5 * lane_sums(jnp.square(fresh).reshape(2 * ROWS, 512))

    square = lax.fori_loop(0, STEPS, step, first_square)
    last = pair(square, square)
    for phase in range(2):
        sum_start(STEPS, phase, last)
        last = sum_end(STEPS, phase)
    norm = last[:, 64:65]
    out[0] = f[zh] / jnp.sqrt(norm / total_size + 1e-06)

    first[0].wait_send()
    arrived(rs_in.at[:, :, :, pl.ds(0, 3)], ag_send.at[0])
    arrived(rs_in.at[:, 0, :, pl.ds(0, 1)], ag_send.at[0])
    arrived(rs_in.at[:, :, :, pl.ds(0, 3)], rs_send.at[0])
    arrived(rs_in.at[:, 0, :, pl.ds(0, 1)], rs_send.at[0])
    arrived(z_in, z_send.at[0])
    for phase in range(2):
        arrived(sc_in[phase].at[:, pl.ds(0, SLOTS[phase] - 1)], sc_send.at[0])

    @pl.when(has_upper)
    def _():
        arrived(blocks.at[:, 0], nb_send.at[0])

    @pl.when(has_lower)
    def _():
        arrived(blocks.at[:, 0], nb_send.at[1])


def per_device(wave, left_ops, right_ops, charges, diag):
    total_size = float(lax.axis_size("sector") * 512 * 512)
    vmem = pl.BlockSpec(memory_space=pltpu.VMEM)
    hbm = pl.BlockSpec(memory_space=pl.ANY)
    dma = pltpu.SemaphoreType.DMA
    return pl.pallas_call(
        functools.partial(kernel, total_size),
        out_shape=jax.ShapeDtypeStruct(wave.shape, F32),
        in_specs=[pl.BlockSpec(memory_space=pltpu.SMEM), hbm, hbm, hbm, hbm],
        out_specs=vmem,
        scratch_shapes=[
            pltpu.VMEM((4, 2, 8, ROWS, 512), BF16),
            pltpu.VMEM((4, 512, 512), BF16),
            pltpu.VMEM((STEPS, 3, 2, 8, ROWS, 512), BF16),
            pltpu.VMEM((2, 8, ROWS, 512), F32),
            pltpu.VMEM((STEPS, 2, 2, 4, ROWS, 512), BF16),
            pltpu.VMEM((STEPS, 2, 2, 4, ROWS, 512), BF16),
            pltpu.VMEM((STEPS, 2, ROWS, 512), BF16),
            pltpu.VMEM((STEPS, 2, ROWS, 512), BF16),
            pltpu.VMEM((2, ROWS, 512), F32),
            pltpu.VMEM((2, ROWS, 512), F32),
            pltpu.VMEM((STEPS + 1, 2, 1, 128), F32),
            pltpu.VMEM((STEPS + 1, SLOTS[0], 1, 128), F32),
            pltpu.VMEM((STEPS + 1, SLOTS[1], 1, 128), F32),
            dma((4,)),
            dma((3,)),
            dma((3,)),
            dma((1,)),
            dma((STEPS, 2, 2, 4)),
            dma((2,)),
            dma((STEPS, 2)),
            dma((1,)),
            dma((STEPS, 2, 2, 4)),
            dma((1,)),
            dma((STEPS,)),
            dma((1,)),
            dma((STEPS + 1, 2)),
        ],
        compiler_params=pltpu.CompilerParams(
            collective_id=0, has_side_effects=True, vmem_limit_bytes=67043328
        ),
        name="sweep",
    )(
        charges,
        wave,
        diag,
        left_ops.reshape(4, 2, 8, ROWS, 512),
        right_ops.reshape(4, 512, 512),
    )


def solution(mesh):
    in_specs = (
        P("sector", "term", None),
        P("term", "sector", None, None),
        P("term", "sector", None, None),
        P(),
        P("sector", "term", None),
    )
    out_specs = P("sector", "term", None)
    return jax.shard_map(
        per_device, mesh=mesh, in_specs=in_specs, out_specs=out_specs, check_vma=False
    )
```

```python
import functools

import jax
import jax.numpy as jnp
from jax import lax
from jax.experimental import pallas as pl
from jax.experimental.pallas import tpu as pltpu
from jax.sharding import PartitionSpec as P

STEPS = 3
SLOTS = (16, 32)


def hops(offset, count):
    return min(offset % count, -offset % count)


ORDER = (
    sorted(range(1, 16), key=lambda o: -hops((o + 1) // 2, 8)),
    sorted(range(1, 32), key=lambda o: -hops(o // 4, 8) - hops(o, 4)),
)
ROWS = 32
BF16, F32 = jnp.bfloat16, jnp.float32
LONG = ((0, 0), (1, 1))
SHORT = ((0, 1), (1, 0))


def wrapped(value, count):
    return lax.rem(value + count, count)


def lane_sums(x):
    x = jnp.sum(x, axis=0, keepdims=True)
    return x[:, :128] + x[:, 128:256] + x[:, 256:384] + x[:, 384:]


def kernel(
    total_size,
    charges,
    wave_hbm,
    diag_hbm,
    left_hbm,
    right_hbm,
    out,
    left,
    right,
    blocks,
    image,
    rs_out,
    rs_in,
    z_out,
    z_in,
    f,
    dg,
    sc_out,
    sc_in_0,
    sc_in_1,
    load_sem,
    first_send,
    first_recv,
    ag_send,
    ag_recv,
    nb_send,
    nb_recv,
    rs_send,
    rs_recv,
    z_send,
    z_recv,
    sc_send,
    sc_recv,
):
    s, t = lax.axis_index("sector"), lax.axis_index("term")
    sectors = lax.axis_size("sector")
    y, zh = lax.rem(t, 8), lax.div(t, 8)
    core, x, zl = lax.rem(s, 2), lax.rem(lax.div(s, 2), 4), lax.div(s, 8)
    z = zh * 4 + zl

    sc_in = (sc_in_0, sc_in_1)

    def remote(src, dst, send, recv, sector, term):
        return pltpu.make_async_remote_copy(
            src_ref=src,
            dst_ref=dst,
            send_sem=send,
            recv_sem=recv,
            device_id={"sector": sector, "term": term},
            device_id_type=pl.DeviceIdType.MESH,
        )

    def arrived(ref, sem):
        pltpu.make_async_copy(ref, ref, sem).wait()

    def peer(phase, offset):
        if phase == 0:
            other = lax.rem(place[0] + offset, 16)
            return s - core + lax.rem(other, 2), zh * 8 + lax.div(other, 2)
        other = lax.rem(place[1] + offset, 32)
        oz = lax.div(other, 4)
        return (lax.rem(oz, 4) * 4 + lax.rem(other, 4)) * 2 + core, lax.div(oz, 4) * 8 + y

    place = (y * 2 + core, z * 4 + x)
    has_lower, has_upper = s > 0, s < sectors - 1

    own = [
        pltpu.make_async_copy(wave_hbm.at[0], f.at[zh], load_sem.at[2]),
        pltpu.make_async_copy(diag_hbm.at[0], dg.at[zh], load_sem.at[3]),
    ]
    loads = [
        pltpu.make_async_copy(left_hbm, left, load_sem.at[0]),
        pltpu.make_async_copy(right_hbm, right, load_sem.at[1]),
    ]
    for load in own + loads:
        load.start()

    barrier = pltpu.get_barrier_semaphore()

    def greet(sector, term):
        pl.semaphore_signal(
            barrier,
            inc=1,
            device_id={"sector": sector, "term": term},
            device_id_type=pl.DeviceIdType.MESH,
        )

    for phase in range(2):

        def greet_peer(offset, carry, phase=phase):
            greet(*peer(phase, offset))
            return carry

        lax.fori_loop(1, SLOTS[phase], greet_peer, 0)
    zt = (1 - zh) * 8 + y
    ring_to = (zh * 8 + wrapped(y + 1, 8), zh * 8 + wrapped(y - 1, 8))
    skip_to = (zh * 8 + wrapped(y + 2, 8), zh * 8 + wrapped(y - 2, 8))
    cross_to = ((1 - zh) * 8 + wrapped(y + 1, 8), (1 - zh) * 8 + wrapped(y - 1, 8))
    for term in cross_to:
        greet(s, term)
    far_lower = jnp.logical_and(core == 0, has_lower)
    far_upper = jnp.logical_and(core == 1, has_upper)

    @pl.when(far_lower)
    def _():
        greet(s - 1, t)

    @pl.when(far_upper)
    def _():
        greet(s + 1, t)

    @pl.when(s == 0)
    def _():
        for k in range(STEPS):
            blocks[k, 2] = jnp.zeros(blocks.shape[2:], BF16)

    @pl.when(s == sectors - 1)
    def _():
        for k in range(STEPS):
            blocks[k, 0] = jnp.zeros(blocks.shape[2:], BF16)

    for load in own:
        load.wait()
    blocks[0, 1, zh, y] = f[zh].astype(BF16)
    first_square = lane_sums(jnp.square(f[zh]))
    pl.semaphore_wait(barrier, 48 + far_lower.astype(jnp.int32) + far_upper.astype(jnp.int32))

    first = [
        remote(blocks.at[0, 1, zh, y], blocks.at[0, 1, zh, y], first_send.at[0], first_recv.at[0], s, zt),
        remote(f.at[zh], f.at[zh], first_send.at[1], first_recv.at[1], s, zt),
        remote(dg.at[zh], dg.at[zh], first_send.at[2], first_recv.at[2], s, zt),
    ]

    def position(d, distance):
        return wrapped(y - distance if d == 0 else y + distance, 8)

    def destination(d, distance):
        return wrapped(y + distance if d == 0 else y - distance, 8)

    def hand_on(k, ref_of):
        @pl.when(has_upper)
        def _():
            remote(ref_of(blocks.at[k, 1]), ref_of(blocks.at[k, 2]), nb_send.at[0], nb_recv.at[k, 0], s + 1, t).start()

        @pl.when(has_lower)
        def _():
            remote(ref_of(blocks.at[k, 1]), ref_of(blocks.at[k, 0]), nb_send.at[1], nb_recv.at[k, 1], s - 1, t).start()

    def gather(k):
        def ring_copy(d, h, r):
            piece = blocks.at[k, 1, h, position(d, r)]
            return remote(piece, piece, ag_send.at[0], ag_recv.at[k, d, h, r], s, ring_to[d])

        def wait_piece(d, h, r):
            ring_copy(d, h, r).wait_recv()

        def start_skip(d, h):
            piece = blocks.at[k, 1, h, position(d, 2)]
            remote(piece, piece, ag_send.at[0], ag_recv.at[k, d, h, 3], s, skip_to[d]).start()

        @pl.when(k == 0)
        def _():
            piece = blocks.at[0, 1, zh, y]
            for d in range(2):
                remote(piece, piece, ag_send.at[0], ag_recv.at[0, d, zh, 0], s, cross_to[d]).start()
            first[0].start()
            for d in range(2):
                remote(piece, piece, ag_send.at[0], ag_recv.at[0, d, zh, 0], s, ring_to[d]).start()
            for copy in first[1:]:
                copy.start()

        @pl.when(k > 0)
        def _():
            for d, h in LONG + SHORT:
                ring_copy(d, h, 0).start()
            hand_on(k, lambda ref: ref.at[:, y])

        for d, h in LONG + SHORT:
            wait_piece(d, h, 0)
            ring_copy(d, h, 1).start()

        @pl.when(k == 0)
        def _():
            first[0].wait_recv()
            hand_on(k, lambda ref: ref.at[:, y])

        for d in range(2):
            hand_on(k, lambda ref: ref.at[:, position(d, 1)])
        for d, h in LONG:
            wait_piece(d, h, 1)
            start_skip(d, h)
            ring_copy(d, h, 2).start()
        for d, h in SHORT:
            wait_piece(d, h, 1)
            ring_copy(d, h, 2).start()
        for d in range(2):
            hand_on(k, lambda ref: ref.at[:, position(d, 2)])
        for d in range(2):
            for h in range(2):
                wait_piece(d, h, 2)
            hand_on(k, lambda ref: ref.at[:, position(d, 3)])
        for d, h in LONG:
            wait_piece(d, h, 3)
        hand_on(k, lambda ref: ref.at[:, position(0, 4)])

        @pl.when(has_lower)
        def _():
            arrived(blocks.at[k, 2], nb_recv.at[k, 0])

        @pl.when(has_upper)
        def _():
            arrived(blocks.at[k, 0], nb_recv.at[k, 1])

    def apply_rows(k, ends):
        total = None
        for i in range(4):
            source = blocks[k, charges[t * 4 + i] + 1].reshape(512, 512)
            rows = jnp.concatenate([left[i, h, e] for e in ends for h in range(2)], axis=0)
            inner = jnp.dot(rows, source, preferred_element_type=F32).astype(BF16)
            term = lax.dot_general(inner, right[i], (((1,), (1,)), ((), ())), preferred_element_type=F32)
            total = term if total is None else total + term
        mine = jnp.concatenate([blocks[k, 1, h, e] for e in ends for h in range(2)], axis=0)
        for j, e in enumerate(ends):
            for h in range(2):
                at = (2 * j + h) * ROWS
                image[h, e] = total[at : at + ROWS]
        return lane_sums(total * mine.astype(F32))

    def pass_on(k, d, h, q):
        value = image[h, destination(d, q)]
        if q == 2:
            rs_copy(k, d, h, 3).wait_recv()
            value = value + rs_in[k, d, h, 2].astype(F32)
            if (d, h) in LONG:
                rs_copy(k, d, h, 4).wait_recv()
                value = value + rs_in[k, d, h, 3].astype(F32)
        rs_out[k, d, h, q - 1] = value.astype(BF16)
        rs_copy(k, d, h, q).start()

    def rs_copy(k, d, h, q):
        return remote(
            rs_out.at[k, d, h, q - 1],
            rs_in.at[k, d, h, q - 1],
            rs_send.at[0],
            rs_recv.at[k, d, h, q - 1],
            s,
            skip_to[d] if q % 2 == 0 else ring_to[d],
        )

    def sum_start(k, phase, values):
        sums = sc_in[phase]
        sc_out[k, phase] = values
        sums[k, place[phase]] = values

        for offset in ORDER[phase]:
            remote(
                sc_out.at[k, phase],
                sums.at[k, place[phase]],
                sc_send.at[0],
                sc_recv.at[k, phase],
                *peer(phase, offset),
            ).start()

    def sum_end(k, phase):
        sums = sc_in[phase]
        arrived(sums.at[k, pl.ds(0, SLOTS[phase] - 1)], sc_recv.at[k, phase])
        return jnp.sum(sums[k], axis=0)

    def pair(cross, square):
        lane = lax.broadcasted_iota(jnp.int32, (1, 128), 1)
        cross, square = (jnp.sum(v, axis=1, keepdims=True) for v in (cross, square))
        return jnp.where(lane < 64, cross, square)

    def step(k, square):
        gather(k)

        @pl.when(k == 0)
        def _():
            for load in loads:
                load.wait()

        cross = apply_rows(k, (destination(0, 4), destination(0, 3), destination(1, 3), destination(0, 2)))
        for d, h in LONG:
            pass_on(k, d, h, 4)
        for d in range(2):
            for h in range(2):
                pass_on(k, d, h, 3)
        cross += apply_rows(k, (destination(1, 2), destination(0, 1), destination(1, 1), y))
        sum_start(k, 0, pair(cross, square))
        for d, h in SHORT + LONG:
            pass_on(k, d, h, 2)
        for d in range(2):
            for h in range(2):
                pass_on(k, d, h, 1)
        sum_start(k, 1, sum_end(k, 0))
        for h in range(2):
            total = image[h, y]
            for d in range(2):
                for q in (1, 2):
                    rs_copy(k, d, h, q).wait_recv()
                    total = total + rs_in[k, d, h, q - 1].astype(F32)
            z_out[k, h] = total.astype(BF16)
        across = remote(z_out.at[k], z_in.at[k], z_send.at[0], z_recv.at[k], s, zt)
        across.start()
        sums = sum_end(k, 1)
        cross_total, square_total = sums[:, 0:1], sums[:, 64:65]
        theta = (cross_total / square_total)[None]
        scale = jnp.where(k == 0, 1.0, 1.0 / jnp.sqrt(square_total / total_size + 1e-06))[None]

        @pl.when(k == 0)
        def _():
            first[1].wait()
            first[2].wait()

        across.wait_recv()
        hpsi = (z_out[k].astype(F32) + z_in[k].astype(F32)) * scale
        psi = f[...] * scale
        fresh = psi - (hpsi - theta * psi) / jnp.maximum(jnp.abs(dg[...] - theta), 1.0)
        f[...] = fresh

        @pl.when(k < STEPS - 1)
        def _():
            blocks[jnp.minimum(k + 1, STEPS - 1), 1, :, y] = fresh.astype(BF16)

        return 0.5 * lane_sums(jnp.square(fresh).reshape(2 * ROWS, 512))

    square = lax.fori_loop(0, STEPS, step, first_square)
    last = pair(square, square)
    for phase in range(2):
        sum_start(STEPS, phase, last)
        last = sum_end(STEPS, phase)
    norm = last[:, 64:65]
    out[0] = f[zh] / jnp.sqrt(norm / total_size + 1e-06)

    first[0].wait_send()
    arrived(rs_in.at[:, :, :, pl.ds(0, 3)], ag_send.at[0])
    arrived(rs_in.at[:, 0, :, pl.ds(0, 1)], ag_send.at[0])
    arrived(rs_in.at[:, :, :, pl.ds(0, 3)], rs_send.at[0])
    arrived(rs_in.at[:, 0, :, pl.ds(0, 1)], rs_send.at[0])
    arrived(z_in, z_send.at[0])
    for phase in range(2):
        arrived(sc_in[phase].at[:, pl.ds(0, SLOTS[phase] - 1)], sc_send.at[0])

    @pl.when(has_upper)
    def _():
        arrived(blocks.at[:, 0], nb_send.at[0])

    @pl.when(has_lower)
    def _():
        arrived(blocks.at[:, 0], nb_send.at[1])


def per_device(wave, left_ops, right_ops, charges, diag):
    total_size = float(lax.axis_size("sector") * 512 * 512)
    vmem = pl.BlockSpec(memory_space=pltpu.VMEM)
    hbm = pl.BlockSpec(memory_space=pl.ANY)
    dma = pltpu.SemaphoreType.DMA
    return pl.pallas_call(
        functools.partial(kernel, total_size),
        out_shape=jax.ShapeDtypeStruct(wave.shape, F32),
        in_specs=[pl.BlockSpec(memory_space=pltpu.SMEM), hbm, hbm, hbm, hbm],
        out_specs=vmem,
        scratch_shapes=[
            pltpu.VMEM((4, 2, 8, ROWS, 512), BF16),
            pltpu.VMEM((4, 512, 512), BF16),
            pltpu.VMEM((STEPS, 3, 2, 8, ROWS, 512), BF16),
            pltpu.VMEM((2, 8, ROWS, 512), F32),
            pltpu.VMEM((STEPS, 2, 2, 4, ROWS, 512), BF16),
            pltpu.VMEM((STEPS, 2, 2, 4, ROWS, 512), BF16),
            pltpu.VMEM((STEPS, 2, ROWS, 512), BF16),
            pltpu.VMEM((STEPS, 2, ROWS, 512), BF16),
            pltpu.VMEM((2, ROWS, 512), F32),
            pltpu.VMEM((2, ROWS, 512), F32),
            pltpu.VMEM((STEPS + 1, 2, 1, 128), F32),
            pltpu.VMEM((STEPS + 1, SLOTS[0], 1, 128), F32),
            pltpu.VMEM((STEPS + 1, SLOTS[1], 1, 128), F32),
            dma((4,)),
            dma((3,)),
            dma((3,)),
            dma((1,)),
            dma((STEPS, 2, 2, 4)),
            dma((2,)),
            dma((STEPS, 2)),
            dma((1,)),
            dma((STEPS, 2, 2, 4)),
            dma((1,)),
            dma((STEPS,)),
            dma((1,)),
            dma((STEPS + 1, 2)),
        ],
        compiler_params=pltpu.CompilerParams(
            collective_id=0, has_side_effects=True, vmem_limit_bytes=67043328
        ),
        name="sweep",
    )(
        charges,
        wave,
        diag,
        left_ops.reshape(4, 2, 8, ROWS, 512),
        right_ops.reshape(4, 512, 512),
    )


def solution(mesh):
    in_specs = (
        P("sector", "term", None),
        P("term", "sector", None, None),
        P("term", "sector", None, None),
        P(),
        P("sector", "term", None),
    )
    out_specs = P("sector", "term", None)
    return jax.shard_map(
        per_device, mesh=mesh, in_specs=in_specs, out_specs=out_specs, check_vma=False
    )
```

```python
import functools

import jax
import jax.numpy as jnp
from jax import lax
from jax.experimental import pallas as pl
from jax.experimental.pallas import tpu as pltpu
from jax.sharding import PartitionSpec as P

STEPS = 3
SLOTS = (16, 32)


def hops(offset, count):
    return min(offset % count, -offset % count)


ORDER = (
    sorted(range(1, 16), key=lambda o: -hops((o + 1) // 2, 8)),
    sorted(range(1, 32), key=lambda o: -hops(o // 4, 8) - hops(o, 4)),
)
ROWS = 32
BF16, F32 = jnp.bfloat16, jnp.float32
LONG = ((0, 0), (1, 1))
SHORT = ((0, 1), (1, 0))


def wrapped(value, count):
    return lax.rem(value + count, count)


def lane_sums(x):
    x = jnp.sum(x, axis=0, keepdims=True)
    return x[:, :128] + x[:, 128:256] + x[:, 256:384] + x[:, 384:]


def kernel(
    total_size,
    charges,
    wave_hbm,
    diag_hbm,
    left_hbm,
    right_hbm,
    out,
    left,
    right,
    blocks,
    image,
    rs_out,
    rs_in,
    z_out,
    z_in,
    f,
    dg,
    sc_out,
    sc_in_0,
    sc_in_1,
    load_sem,
    first_send,
    first_recv,
    ag_send,
    ag_recv,
    nb_send,
    nb_recv,
    rs_send,
    rs_recv,
    z_send,
    z_recv,
    sc_send,
    sc_recv,
):
    s, t = lax.axis_index("sector"), lax.axis_index("term")
    sectors = lax.axis_size("sector")
    y, zh = lax.rem(t, 8), lax.div(t, 8)
    core, x, zl = lax.rem(s, 2), lax.rem(lax.div(s, 2), 4), lax.div(s, 8)
    z = zh * 4 + zl

    sc_in = (sc_in_0, sc_in_1)

    def remote(src, dst, send, recv, sector, term):
        return pltpu.make_async_remote_copy(
            src_ref=src,
            dst_ref=dst,
            send_sem=send,
            recv_sem=recv,
            device_id={"sector": sector, "term": term},
            device_id_type=pl.DeviceIdType.MESH,
        )

    def arrived(ref, sem):
        pltpu.make_async_copy(ref, ref, sem).wait()

    def peer(phase, offset):
        if phase == 0:
            other = lax.rem(place[0] + offset, 16)
            return s - core + lax.rem(other, 2), zh * 8 + lax.div(other, 2)
        other = lax.rem(place[1] + offset, 32)
        oz = lax.div(other, 4)
        return (lax.rem(oz, 4) * 4 + lax.rem(other, 4)) * 2 + core, lax.div(oz, 4) * 8 + y

    place = (y * 2 + core, z * 4 + x)
    has_lower, has_upper = s > 0, s < sectors - 1

    own = [
        pltpu.make_async_copy(wave_hbm.at[0], f.at[zh], load_sem.at[2]),
        pltpu.make_async_copy(diag_hbm.at[0], dg.at[zh], load_sem.at[3]),
    ]
    loads = [
        pltpu.make_async_copy(left_hbm, left, load_sem.at[0]),
        pltpu.make_async_copy(right_hbm, right, load_sem.at[1]),
    ]
    for load in own + loads:
        load.start()

    barrier = pltpu.get_barrier_semaphore()

    def greet(sector, term):
        pl.semaphore_signal(
            barrier,
            inc=1,
            device_id={"sector": sector, "term": term},
            device_id_type=pl.DeviceIdType.MESH,
        )

    for phase in (1, 0):
        for offset in ORDER[phase]:
            greet(*peer(phase, offset))
    zt = (1 - zh) * 8 + y
    ring_to = (zh * 8 + wrapped(y + 1, 8), zh * 8 + wrapped(y - 1, 8))
    skip_to = (zh * 8 + wrapped(y + 2, 8), zh * 8 + wrapped(y - 2, 8))
    cross_to = ((1 - zh) * 8 + wrapped(y + 1, 8), (1 - zh) * 8 + wrapped(y - 1, 8))
    for term in cross_to:
        greet(s, term)
    far_lower = jnp.logical_and(core == 0, has_lower)
    far_upper = jnp.logical_and(core == 1, has_upper)

    @pl.when(far_lower)
    def _():
        greet(s - 1, t)

    @pl.when(far_upper)
    def _():
        greet(s + 1, t)

    @pl.when(s == 0)
    def _():
        for k in range(STEPS):
            blocks[k, 2] = jnp.zeros(blocks.shape[2:], BF16)

    @pl.when(s == sectors - 1)
    def _():
        for k in range(STEPS):
            blocks[k, 0] = jnp.zeros(blocks.shape[2:], BF16)

    for load in own:
        load.wait()
    blocks[0, 1, zh, y] = f[zh].astype(BF16)
    first_square = lane_sums(jnp.square(f[zh]))
    pl.semaphore_wait(barrier, 48 + far_lower.astype(jnp.int32) + far_upper.astype(jnp.int32))

    first = [
        remote(blocks.at[0, 1, zh, y], blocks.at[0, 1, zh, y], first_send.at[0], first_recv.at[0], s, zt),
        remote(f.at[zh], f.at[zh], first_send.at[1], first_recv.at[1], s, zt),
        remote(dg.at[zh], dg.at[zh], first_send.at[2], first_recv.at[2], s, zt),
    ]

    def position(d, distance):
        return wrapped(y - distance if d == 0 else y + distance, 8)

    def destination(d, distance):
        return wrapped(y + distance if d == 0 else y - distance, 8)

    def hand_on(k, ref_of):
        @pl.when(has_upper)
        def _():
            remote(ref_of(blocks.at[k, 1]), ref_of(blocks.at[k, 2]), nb_send.at[0], nb_recv.at[k, 0], s + 1, t).start()

        @pl.when(has_lower)
        def _():
            remote(ref_of(blocks.at[k, 1]), ref_of(blocks.at[k, 0]), nb_send.at[1], nb_recv.at[k, 1], s - 1, t).start()

    def gather(k):
        def ring_copy(d, h, r):
            piece = blocks.at[k, 1, h, position(d, r)]
            return remote(piece, piece, ag_send.at[0], ag_recv.at[k, d, h, r], s, ring_to[d])

        def wait_piece(d, h, r):
            ring_copy(d, h, r).wait_recv()

        def start_skip(d, h):
            piece = blocks.at[k, 1, h, position(d, 2)]
            remote(piece, piece, ag_send.at[0], ag_recv.at[k, d, h, 3], s, skip_to[d]).start()

        @pl.when(k == 0)
        def _():
            piece = blocks.at[0, 1, zh, y]
            for d in range(2):
                remote(piece, piece, ag_send.at[0], ag_recv.at[0, d, zh, 0], s, cross_to[d]).start()
            first[0].start()
            for d in range(2):
                remote(piece, piece, ag_send.at[0], ag_recv.at[0, d, zh, 0], s, ring_to[d]).start()
            for copy in first[1:]:
                copy.start()

        @pl.when(k > 0)
        def _():
            for d, h in LONG + SHORT:
                ring_copy(d, h, 0).start()
            hand_on(k, lambda ref: ref.at[:, y])

        for d, h in LONG + SHORT:
            wait_piece(d, h, 0)
            ring_copy(d, h, 1).start()

        @pl.when(k == 0)
        def _():
            first[0].wait_recv()
            hand_on(k, lambda ref: ref.at[:, y])

        for d in range(2):
            hand_on(k, lambda ref: ref.at[:, position(d, 1)])
        for d, h in LONG:
            wait_piece(d, h, 1)
            start_skip(d, h)
            ring_copy(d, h, 2).start()
        for d, h in SHORT:
            wait_piece(d, h, 1)
            ring_copy(d, h, 2).start()
        for d in range(2):
            hand_on(k, lambda ref: ref.at[:, position(d, 2)])
        for d in range(2):
            for h in range(2):
                wait_piece(d, h, 2)
            hand_on(k, lambda ref: ref.at[:, position(d, 3)])
        for d, h in LONG:
            wait_piece(d, h, 3)
        hand_on(k, lambda ref: ref.at[:, position(0, 4)])

        @pl.when(has_lower)
        def _():
            arrived(blocks.at[k, 2], nb_recv.at[k, 0])

        @pl.when(has_upper)
        def _():
            arrived(blocks.at[k, 0], nb_recv.at[k, 1])

    def apply_rows(k, ends):
        total = None
        for i in range(4):
            source = blocks[k, charges[t * 4 + i] + 1].reshape(512, 512)
            rows = jnp.concatenate([left[i, h, e] for e in ends for h in range(2)], axis=0)
            inner = jnp.dot(rows, source, preferred_element_type=F32).astype(BF16)
            term = lax.dot_general(inner, right[i], (((1,), (1,)), ((), ())), preferred_element_type=F32)
            total = term if total is None else total + term
        mine = jnp.concatenate([blocks[k, 1, h, e] for e in ends for h in range(2)], axis=0)
        for j, e in enumerate(ends):
            for h in range(2):
                at = (2 * j + h) * ROWS
                image[h, e] = total[at : at + ROWS]
        return lane_sums(total * mine.astype(F32))

    def pass_on(k, d, h, q):
        value = image[h, destination(d, q)]
        if q == 2:
            rs_copy(k, d, h, 3).wait_recv()
            value = value + rs_in[k, d, h, 2].astype(F32)
            if (d, h) in LONG:
                rs_copy(k, d, h, 4).wait_recv()
                value = value + rs_in[k, d, h, 3].astype(F32)
        rs_out[k, d, h, q - 1] = value.astype(BF16)
        rs_copy(k, d, h, q).start()

    def rs_copy(k, d, h, q):
        return remote(
            rs_out.at[k, d, h, q - 1],
            rs_in.at[k, d, h, q - 1],
            rs_send.at[0],
            rs_recv.at[k, d, h, q - 1],
            s,
            skip_to[d] if q % 2 == 0 else ring_to[d],
        )

    def sum_start(k, phase, values):
        sums = sc_in[phase]
        sc_out[k, phase] = values
        sums[k, place[phase]] = values

        for offset in ORDER[phase]:
            remote(
                sc_out.at[k, phase],
                sums.at[k, place[phase]],
                sc_send.at[0],
                sc_recv.at[k, phase],
                *peer(phase, offset),
            ).start()

    def sum_end(k, phase):
        sums = sc_in[phase]
        arrived(sums.at[k, pl.ds(0, SLOTS[phase] - 1)], sc_recv.at[k, phase])
        return jnp.sum(sums[k], axis=0)

    def pair(cross, square):
        lane = lax.broadcasted_iota(jnp.int32, (1, 128), 1)
        cross, square = (jnp.sum(v, axis=1, keepdims=True) for v in (cross, square))
        return jnp.where(lane < 64, cross, square)

    def step(k, square):
        gather(k)

        @pl.when(k == 0)
        def _():
            for load in loads:
                load.wait()

        cross = apply_rows(k, (destination(0, 4), destination(0, 3), destination(1, 3), destination(0, 2)))
        for d, h in LONG:
            pass_on(k, d, h, 4)
        for d in range(2):
            for h in range(2):
                pass_on(k, d, h, 3)
        cross += apply_rows(k, (destination(1, 2), destination(0, 1), destination(1, 1), y))
        sum_start(k, 0, pair(cross, square))
        for d in range(2):
            for h in range(2):
                pass_on(k, d, h, 1)
        for d, h in SHORT + LONG:
            pass_on(k, d, h, 2)
        sum_start(k, 1, sum_end(k, 0))
        for h in range(2):
            total = image[h, y]
            for d in range(2):
                for q in (1, 2):
                    rs_copy(k, d, h, q).wait_recv()
                    total = total + rs_in[k, d, h, q - 1].astype(F32)
            z_out[k, h] = total.astype(BF16)
        across = remote(z_out.at[k], z_in.at[k], z_send.at[0], z_recv.at[k], s, zt)
        across.start()
        sums = sum_end(k, 1)
        cross_total, square_total = sums[:, 0:1], sums[:, 64:65]
        theta = (cross_total / square_total)[None]
        scale = jnp.where(k == 0, 1.0, 1.0 / jnp.sqrt(square_total / total_size + 1e-06))[None]

        @pl.when(k == 0)
        def _():
            first[1].wait()
            first[2].wait()

        across.wait_recv()
        hpsi = (z_out[k].astype(F32) + z_in[k].astype(F32)) * scale
        psi = f[...] * scale
        fresh = psi - (hpsi - theta * psi) / jnp.maximum(jnp.abs(dg[...] - theta), 1.0)
        f[...] = fresh

        @pl.when(k < STEPS - 1)
        def _():
            blocks[jnp.minimum(k + 1, STEPS - 1), 1, :, y] = fresh.astype(BF16)

        return 0.5 * lane_sums(jnp.square(fresh).reshape(2 * ROWS, 512))

    square = lax.fori_loop(0, STEPS, step, first_square)
    last = pair(square, square)
    for phase in range(2):
        sum_start(STEPS, phase, last)
        last = sum_end(STEPS, phase)
    norm = last[:, 64:65]
    out[0] = f[zh] / jnp.sqrt(norm / total_size + 1e-06)

    first[0].wait_send()
    arrived(rs_in.at[:, :, :, pl.ds(0, 3)], ag_send.at[0])
    arrived(rs_in.at[:, 0, :, pl.ds(0, 1)], ag_send.at[0])
    arrived(rs_in.at[:, :, :, pl.ds(0, 3)], rs_send.at[0])
    arrived(rs_in.at[:, 0, :, pl.ds(0, 1)], rs_send.at[0])
    arrived(z_in, z_send.at[0])
    for phase in range(2):
        arrived(sc_in[phase].at[:, pl.ds(0, SLOTS[phase] - 1)], sc_send.at[0])

    @pl.when(has_upper)
    def _():
        arrived(blocks.at[:, 0], nb_send.at[0])

    @pl.when(has_lower)
    def _():
        arrived(blocks.at[:, 0], nb_send.at[1])


def per_device(wave, left_ops, right_ops, charges, diag):
    total_size = float(lax.axis_size("sector") * 512 * 512)
    vmem = pl.BlockSpec(memory_space=pltpu.VMEM)
    hbm = pl.BlockSpec(memory_space=pl.ANY)
    dma = pltpu.SemaphoreType.DMA
    return pl.pallas_call(
        functools.partial(kernel, total_size),
        out_shape=jax.ShapeDtypeStruct(wave.shape, F32),
        in_specs=[pl.BlockSpec(memory_space=pltpu.SMEM), hbm, hbm, hbm, hbm],
        out_specs=vmem,
        scratch_shapes=[
            pltpu.VMEM((4, 2, 8, ROWS, 512), BF16),
            pltpu.VMEM((4, 512, 512), BF16),
            pltpu.VMEM((STEPS, 3, 2, 8, ROWS, 512), BF16),
            pltpu.VMEM((2, 8, ROWS, 512), F32),
            pltpu.VMEM((STEPS, 2, 2, 4, ROWS, 512), BF16),
            pltpu.VMEM((STEPS, 2, 2, 4, ROWS, 512), BF16),
            pltpu.VMEM((STEPS, 2, ROWS, 512), BF16),
            pltpu.VMEM((STEPS, 2, ROWS, 512), BF16),
            pltpu.VMEM((2, ROWS, 512), F32),
            pltpu.VMEM((2, ROWS, 512), F32),
            pltpu.VMEM((STEPS + 1, 2, 1, 128), F32),
            pltpu.VMEM((STEPS + 1, SLOTS[0], 1, 128), F32),
            pltpu.VMEM((STEPS + 1, SLOTS[1], 1, 128), F32),
            dma((4,)),
            dma((3,)),
            dma((3,)),
            dma((1,)),
            dma((STEPS, 2, 2, 4)),
            dma((2,)),
            dma((STEPS, 2)),
            dma((1,)),
            dma((STEPS, 2, 2, 4)),
            dma((1,)),
            dma((STEPS,)),
            dma((1,)),
            dma((STEPS + 1, 2)),
        ],
        compiler_params=pltpu.CompilerParams(
            collective_id=0, has_side_effects=True, vmem_limit_bytes=67043328
        ),
        name="sweep",
    )(
        charges,
        wave,
        diag,
        left_ops.reshape(4, 2, 8, ROWS, 512),
        right_ops.reshape(4, 512, 512),
    )


def solution(mesh):
    in_specs = (
        P("sector", "term", None),
        P("term", "sector", None, None),
        P("term", "sector", None, None),
        P(),
        P("sector", "term", None),
    )
    out_specs = P("sector", "term", None)
    return jax.shard_map(
        per_device, mesh=mesh, in_specs=in_specs, out_specs=out_specs, check_vma=False
    )
```
